256 devices in a mesh: seq: 64 (over x_hi, y, z), tp: 4 (over x_lo, core).
Axes of the slice: x: 4 (x_hi: 2, x_lo: 2; x = x_hi * 2 + x_lo), y: 4, z: 8, core: 2. Of those that a mesh axis runs over, the one named last changes fastest.
Arguments:
- mixer_input: bfloat16 [8192, 8192], P('seq', 'tp'), may hold values from -6 to 6
- gate_input: bfloat16 [8192, 8192], P('seq', 'tp'), may hold values from -6 to 6
- input_matrix: bfloat16 [8192, 1024], P('seq', 'tp'), may hold values from -6 to 6
- output_matrix: bfloat16 [8192, 1024], P('seq', 'tp'), may hold values from -6 to 6
- step_raw: float32 [8192, 128], P('seq', 'tp'), may hold values from -3 to 3
- step_bias: float32 [128], P('tp'), may hold values from -1 to 0.5
- decay_rate: float32 [128], P('tp'), may hold values from 0.0001 to 0.05
- skip_weight: float32 [128], P('tp'), may hold values from 0.5 to 1.5
- conv_mixer: float32 [4, 8192], P(None, 'tp'), may hold values from -3 to 3
- conv_input: float32 [4, 1024], P(None, 'tp'), may hold values from -3 to 3
- conv_output: float32 [4, 1024], P(None, 'tp'), may hold values from -3 to 3
- norm_gain: float32 [8192], P('tp'), may hold values from 0.5 to 1.5
- queries: bfloat16 [8192, 8192], P('seq', 'tp'), may hold values from -5 to 5
- keys: bfloat16 [8192, 1024], P('seq', 'tp'), may hold values from -5 to 5
- values: bfloat16 [8192, 1024], P('seq', 'tp'), may hold values from -6 to 6
Outputs:
- mixer_out: bfloat16 [8192, 8192], P('seq', 'tp')
- attention_out: bfloat16 [8192, 8192], P('seq', 'tp')
The draws below stay inside these ranges and needn't reach their ends.
All inputs are finite; a program needn't handle non-finite values.
Results may differ from the reference program's by a relative error of at most 0.007.
Values may be sent and summed in bfloat16 or wider, within the bound.
No kernel may reach another device: no remote copies, remote signals or barrier semaphores. Data moves between devices by JAX's collectives and lax.ppermute only.
A program may use at most 192 MiB of HBM per device.

```python
import math
import jax
import jax.numpy as jnp
from jax import lax

MH = 128
P_SIZE = 64
STATE = 128
GROUPS = 8
QH = 64
KVH = 8
HD = 128
CONV = 4
SCAN_BLOCK = 128
INNER = 8192
TOKENS = 8192


def draw_queries(key, part):
    drawn = jnp.clip(jax.random.normal(jax.random.fold_in(key, 1), (TOKENS, QH * HD), jnp.float32), -5.0, 5.0)
    return drawn.astype(jnp.bfloat16)


def draw_keys(key, part):
    drawn = jnp.clip(jax.random.normal(jax.random.fold_in(key, 2), (TOKENS, KVH * HD), jnp.float32), -5.0, 5.0)
    return drawn.astype(jnp.bfloat16)


def block_levels(stream_key, shape, cuts, least, top_value):
    factor_of = 1.0
    for dim, parts in cuts:
        draws = jax.random.uniform(jax.random.fold_in(jax.random.fold_in(stream_key, 6), dim), (parts,), jnp.float32, least / len(cuts), top_value / len(cuts))
        factor_of = factor_of * jnp.repeat(jnp.exp(draws), shape[dim] // parts).reshape((-1,) + (1,) * (len(shape) - 1 - dim))
    return factor_of


def normal_values(own_key, extent, width, bound, shards=(), held_as=jnp.bfloat16):
    values = width * jax.random.normal(own_key, extent, jnp.float32)
    if shards:
        values = values * block_levels(own_key, extent, shards, -0.22, 0.18)
    return jnp.clip(values, -bound, bound).astype(held_as)


def setup_inputs(seed: int = 0) -> dict:
    splits = jax.random.split(jax.random.key(seed), 16)
    mixer_input = normal_values(splits[0], (TOKENS, INNER), 1.0, 6.0, ((0, 64), (1, 4)))
    gate_input = normal_values(splits[1], (TOKENS, INNER), 1.0, 6.0, ((0, 64), (1, 4)))
    input_matrix = normal_values(splits[2], (TOKENS, GROUPS * STATE), 1.0, 6.0, ((0, 64), (1, 4)))
    output_matrix = normal_values(splits[3], (TOKENS, GROUPS * STATE), 1.0, 6.0, ((0, 64), (1, 4)))
    step_raw = normal_values(splits[4], (TOKENS, MH), 0.5, 3.0, ((0, 64), (1, 4)), jnp.float32)
    step_bias = jnp.clip(-1.0 + 1.5 * jax.random.uniform(splits[5], (MH,), jnp.float32) ** block_levels(splits[5], (MH,), ((0, 4),), -0.2, 0.2), -1.0, 0.5)
    decay_rate = jnp.clip(jnp.exp(math.log(0.05) - 6.214608 * jax.random.uniform(splits[6], (MH,), jnp.float32) ** block_levels(splits[6], (MH,), ((0, 4),), -0.2, 0.2)), 0.0001, 0.05)
    skip_weight = jnp.clip(0.5 + 1.0 * jax.random.uniform(splits[7], (MH,), jnp.float32) ** block_levels(splits[7], (MH,), ((0, 4),), -0.2, 0.2), 0.5, 1.5)
    conv_mixer = normal_values(splits[8], (CONV, INNER), CONV ** -0.5, 3.0, ((1, 4),), jnp.float32)
    conv_input = normal_values(splits[9], (CONV, GROUPS * STATE), CONV ** -0.5, 3.0, ((1, 4),), jnp.float32)
    conv_output = normal_values(splits[10], (CONV, GROUPS * STATE), CONV ** -0.5, 3.0, ((1, 4),), jnp.float32)
    norm_gain = jnp.clip(1.0 + 0.1 * jax.random.normal(splits[11], (INNER,), jnp.float32), 0.5, 1.5)
    queries = draw_queries(jax.random.fold_in(splits[15], 71), 0)
    keys = draw_keys(jax.random.fold_in(splits[15], 71), 0)
    values = normal_values(splits[14], (TOKENS, KVH * HD), 1.0, 6.0, ((0, 64), (1, 4)))
    return {"mixer_input": mixer_input, "gate_input": gate_input, "input_matrix": input_matrix, "output_matrix": output_matrix, "step_raw": step_raw, "step_bias": step_bias, "decay_rate": decay_rate, "skip_weight": skip_weight, "conv_mixer": conv_mixer, "conv_input": conv_input, "conv_output": conv_output, "norm_gain": norm_gain, "queries": queries, "keys": keys, "values": values}


HIGHEST = lax.Precision.HIGHEST
norm_epsilon = 1e-05
lowest_score = -1e+30

def conv_silu(raw_rows, weights, history):
    padded = jnp.concatenate([history, raw_rows], axis=0).astype(jnp.float32)
    length = raw_rows.shape[0]
    summed = jnp.zeros((length, raw_rows.shape[1]), jnp.float32)
    for offset in range(weights.shape[0]):
        summed = summed + weights[offset][None, :] * padded[offset:offset + length]
    return jax.nn.silu(summed)

def ssd_block(signal, b_state, c_state, step_size, rates, carried):
    group_heads = signal.shape[1] // b_state.shape[1]
    log_decay = jnp.cumsum(-step_size * rates[None, :], axis=0)
    length = signal.shape[0]
    places = jnp.arange(length, dtype=jnp.int32)
    causal = (places[:, None] >= places[None, :])[:, :, None]
    spread = jnp.where(causal, log_decay[:, None, :] - log_decay[None, :, :], 0.0)
    decays = jnp.where(causal, jnp.exp(spread), 0.0)
    coupling = jnp.einsum('tgn,sgn->gts', c_state, b_state, precision=HIGHEST)
    coupling = jnp.repeat(coupling, group_heads, axis=0)
    mixing = jnp.transpose(decays, (2, 0, 1)) * coupling
    scaled = signal * step_size[:, :, None]
    output = jnp.einsum('hts,shp->thp', mixing, scaled, precision=HIGHEST)
    b_heads = jnp.repeat(b_state, group_heads, axis=1)
    c_heads = jnp.repeat(c_state, group_heads, axis=1)
    output = output + jnp.exp(log_decay)[:, :, None] * jnp.einsum('thn,hpn->thp', c_heads, carried, precision=HIGHEST)
    closing = jnp.exp(log_decay[-1][None, :] - log_decay)
    weighted = scaled * closing[:, :, None]
    updated = jnp.exp(log_decay[-1])[:, None, None] * carried + jnp.einsum('shp,shn->hpn', weighted, b_heads, precision=HIGHEST)
    return (output, updated, log_decay, c_heads)

def attend_update(carry, query_block, query_start, key_block, value_block, key_start, widen):
    maxima, totals, accum = carry
    kv_heads = key_block.shape[1] // HD
    grouped = query_block.shape[1] // HD // kv_heads
    query_rows = query_block.shape[0]
    key_rows = key_block.shape[0]
    query_four = query_block.reshape(query_rows, kv_heads, grouped, HD)
    key_three = key_block.reshape(key_rows, kv_heads, HD)
    value_three = value_block.reshape(key_rows, kv_heads, HD)
    if widen:
        scores = jnp.einsum('qhgd,khd->hgqk', query_four.astype(jnp.float32), key_three.astype(jnp.float32))
    else:
        scores = jnp.einsum('qhgd,khd->hgqk', query_four, key_three, preferred_element_type=jnp.float32)
    scores = scores * (1.0 / math.sqrt(HD))
    query_places = query_start + jnp.arange(query_rows, dtype=jnp.int32)
    key_places = key_start + jnp.arange(key_rows, dtype=jnp.int32)
    allowed = key_places[None, :] <= query_places[:, None]
    masked = jnp.where(allowed, scores, lowest_score)
    newmax = jnp.maximum(maxima, lax.optimization_barrier(jnp.max(masked, axis=-1)))
    probs = jnp.where(allowed, jnp.exp(masked - newmax[..., None]), 0.0)
    factor = jnp.exp(maxima - newmax)
    totals = totals * factor + lax.optimization_barrier(jnp.sum(probs, axis=-1))
    rounded = probs.astype(jnp.bfloat16)
    if widen:
        product = jnp.einsum('hgqk,khd->hgqd', rounded.astype(jnp.float32), value_three.astype(jnp.float32))
    else:
        product = jnp.einsum('hgqk,khd->hgqd', rounded, value_three, preferred_element_type=jnp.float32)
    accum = accum * factor[..., None] + product
    return (newmax, totals, accum)

def finish(carry):
    maxima, totals, accum = carry
    result = accum / totals[..., None]
    result = jnp.transpose(result, (2, 0, 1, 3))
    return result.reshape(result.shape[0], -1).astype(jnp.bfloat16)

def attention(queries, keys, values):
    span = math.gcd(TOKENS, 512)
    count = TOKENS // span
    grouped = QH // KVH

    def one_block(index):
        start = index * span
        query_block = lax.dynamic_slice_in_dim(queries, start, span, 0)
        initial = (jnp.full((KVH, grouped, span), lowest_score, jnp.float32), jnp.zeros((KVH, grouped, span), jnp.float32), jnp.zeros((KVH, grouped, span, HD), jnp.float32))

        def visit(position, carry):
            key_start = position * span
            key_block = lax.dynamic_slice_in_dim(keys, key_start, span, 0)
            value_block = lax.dynamic_slice_in_dim(values, key_start, span, 0)
            return attend_update(carry, query_block, start, key_block, value_block, key_start, True)
        return finish(lax.fori_loop(0, index + 1, visit, initial))
    blocks = lax.map(one_block, jnp.arange(count, dtype=jnp.int32))
    return blocks.reshape(TOKENS, QH * HD)

def reference(mixer_input, gate_input, input_matrix, output_matrix, step_raw, step_bias, decay_rate, skip_weight, conv_mixer, conv_input, conv_output, norm_gain, queries, keys, values):
    reach = CONV - 1
    signal = conv_silu(mixer_input, conv_mixer, jnp.zeros((reach, mixer_input.shape[1]), jnp.bfloat16))
    b_state = conv_silu(input_matrix, conv_input, jnp.zeros((reach, input_matrix.shape[1]), jnp.bfloat16))
    c_state = conv_silu(output_matrix, conv_output, jnp.zeros((reach, output_matrix.shape[1]), jnp.bfloat16))
    signal = signal.reshape(TOKENS, MH, P_SIZE)
    b_state = b_state.reshape(TOKENS, GROUPS, STATE)
    c_state = c_state.reshape(TOKENS, GROUPS, STATE)
    step_size = jax.nn.softplus(step_raw + step_bias[None, :])
    blocks = TOKENS // SCAN_BLOCK

    def advance(carried, pieces):
        signal_part, b_part, c_part, step_part = pieces
        output, updated, log_decay, c_heads = ssd_block(signal_part, b_part, c_part, step_part, decay_rate, carried)
        return (updated, output)
    _, outputs = lax.scan(advance, jnp.zeros((MH, P_SIZE, STATE), jnp.float32), (signal.reshape(blocks, SCAN_BLOCK, MH, P_SIZE), b_state.reshape(blocks, SCAN_BLOCK, GROUPS, STATE), c_state.reshape(blocks, SCAN_BLOCK, GROUPS, STATE), step_size.reshape(blocks, SCAN_BLOCK, MH)))
    mixed = outputs.reshape(TOKENS, MH, P_SIZE) + skip_weight[None, :, None] * signal
    gated = mixed.reshape(TOKENS, MH * P_SIZE) * jax.nn.silu(gate_input.astype(jnp.float32))
    squares = lax.optimization_barrier(jnp.mean(gated * gated, axis=1, keepdims=True))
    mixer_out = (gated * lax.rsqrt(squares + norm_epsilon) * norm_gain[None, :]).astype(jnp.bfloat16)
    attention_out = attention(queries, keys, values)
    return (mixer_out, attention_out)
```

```python
import math

import jax
import jax.numpy as jnp
from jax import lax
from jax.experimental import pallas as pl
from jax.experimental.pallas import tpu as pltpu
from jax.sharding import Mesh
from jax.sharding import PartitionSpec as P

MH = 128
P_SIZE = 64
STATE = 128
HD = 128
CONV = 4
LINE = ("xh", "y")
SEQ = ("xh", "y", "z")

norm_epsilon = 1e-05
lowest_score = -1e30
EXP2_SCALE = math.log2(math.e) / math.sqrt(HD)


def conv_silu(raw_rows, weights, history):
    padded = jnp.concatenate([history, raw_rows], axis=0).astype(jnp.float32)
    length = raw_rows.shape[0]
    summed = jnp.zeros((length, raw_rows.shape[1]), jnp.float32)
    for offset in range(weights.shape[0]):
        summed = summed + weights[offset][None, :] * padded[offset : offset + length]
    return jax.nn.silu(summed)


def attend_kernel(z_ref, q_ref, kv_ref, o_ref):
    lines, zs, length = q_ref.shape[0], kv_ref.shape[0], q_ref.shape[1]
    span = zs * length
    rows = 2 * length

    def chunk(g):
        both = kv_ref[:, g].reshape(span, 2 * HD)
        return both[:, :HD], both[:, HD:]

    def scores_of(q, k):
        return lax.dot_general(q, k, (((1,), (1,)), ((), ())), preferred_element_type=jnp.float32)

    def one_line(g, _):
        both = q_ref[g, :, : 2 * HD]
        q = jnp.concatenate([both[:, :HD], both[:, HD:]], axis=0)
        k, v = chunk(g)
        s = scores_of(q, k)
        place = lax.broadcasted_iota(jnp.int32, (rows, span), 0) % length + z_ref[0] * length
        key_place = lax.broadcasted_iota(jnp.int32, (rows, span), 1)
        s = jnp.where(key_place <= place, s, lowest_score)
        m = jnp.max(s, axis=-1, keepdims=True)
        p = jnp.exp2((s - m) * EXP2_SCALE)
        total = jnp.sum(p, axis=-1, keepdims=True)
        acc = jnp.dot(p.astype(jnp.bfloat16), v, preferred_element_type=jnp.float32)

        def visit(other, carry):
            m, total, acc = carry
            k, v = chunk(other)
            s = scores_of(q, k)
            new = jnp.maximum(m, jnp.max(s, axis=-1, keepdims=True))
            p = jnp.exp2((s - new) * EXP2_SCALE)
            factor = jnp.exp2((m - new) * EXP2_SCALE)
            total = total * factor + jnp.sum(p, axis=-1, keepdims=True)
            acc = acc * factor + jnp.dot(
                p.astype(jnp.bfloat16), v, preferred_element_type=jnp.float32
            )
            return new, total, acc

        m, total, acc = lax.fori_loop(0, g, visit, (m, total, acc))
        out = (acc / total).astype(jnp.bfloat16)
        o_ref[g, :, :HD] = out[:length]
        o_ref[g, :, HD:] = out[length:]
        return 0

    lax.fori_loop(0, lines, one_line, 0)


def attend(z, q, kv):
    lines, length = q.shape[0], q.shape[1]
    pairs = lines * (lines + 1) // 2 * 2 * length * kv.shape[0] * length
    return pl.pallas_call(
        attend_kernel,
        out_shape=jax.ShapeDtypeStruct((lines, length, 2 * HD), jnp.bfloat16),
        in_specs=[
            pl.BlockSpec(memory_space=pltpu.SMEM),
            pl.BlockSpec(memory_space=pltpu.VMEM),
            pl.BlockSpec(memory_space=pltpu.VMEM),
        ],
        out_specs=pl.BlockSpec(memory_space=pltpu.VMEM),
        cost_estimate=pl.CostEstimate(
            flops=pairs * HD * 4, bytes_accessed=kv.size * 2 + q.size * 4, transcendentals=pairs
        ),
        compiler_params=pltpu.CompilerParams(vmem_limit_bytes=40 * 1024 * 1024),
        name="attend",
    )(z, q, kv)


def attend_local(queries, keys, values):
    length = queries.shape[0]
    lines = lax.axis_size(LINE)
    kv_heads = keys.shape[1] // HD
    shared = lines // kv_heads
    q = queries.reshape(length, lines, 2 * HD).transpose(1, 0, 2)
    k = keys.reshape(length, kv_heads, HD).transpose(1, 0, 2)
    v = values.reshape(length, kv_heads, HD).transpose(1, 0, 2)
    kv = jnp.repeat(jnp.concatenate([k, v], axis=2), shared, axis=0)
    kv = lax.all_to_all(kv, LINE, 0, 0, tiled=True)
    kv = lax.all_gather(kv, "z")
    q = lax.all_to_all(q, LINE, 0, 0, tiled=True)
    z = lax.axis_index("z").astype(jnp.int32).reshape(1)
    out = attend(z, q, kv)
    out = lax.all_to_all(out, LINE, 0, 0, tiled=True)
    return out.transpose(1, 0, 2).reshape(length, lines * 2 * HD)


def carry_kernel(piece_ref, o_ref):
    count, rows = o_ref.shape[0], o_ref.shape[1]

    def step(j, state):
        o_ref[j] = state.astype(jnp.bfloat16)
        block = piece_ref[j].astype(jnp.float32)
        log = block[rows : rows + 1] + block[rows + 1 : rows + 2] + block[rows + 2 : rows + 3]
        return jnp.exp(log) * state + block[:rows]

    lax.fori_loop(0, count, step, jnp.zeros((rows, STATE), jnp.float32), unroll=8)


def carry_states(pieces):
    count, rows = pieces.shape[0], pieces.shape[1] - 8
    return pl.pallas_call(
        carry_kernel,
        out_shape=jax.ShapeDtypeStruct((count, rows, STATE), jnp.bfloat16),
        in_specs=[pl.BlockSpec(memory_space=pltpu.VMEM)],
        out_specs=pl.BlockSpec(memory_space=pltpu.VMEM),
        cost_estimate=pl.CostEstimate(
            flops=1000000, bytes_accessed=pieces.size * 4, transcendentals=count * 128
        ),
        name="carry_states",
    )(pieces)


def entering_state(own, log_total):
    heads = own.shape[0]
    count = lax.axis_size(SEQ)
    rows = heads * P_SIZE // count
    per_head = count // heads
    body = own.astype(jnp.bfloat16).reshape(count, rows, STATE)
    log = jnp.repeat(log_total, per_head)[:, None, None]
    high = log.astype(jnp.bfloat16)
    rest = log - high.astype(jnp.float32)
    mid = rest.astype(jnp.bfloat16)
    low = (rest - mid.astype(jnp.float32)).astype(jnp.bfloat16)
    which = lax.broadcasted_iota(jnp.int32, (count, 8, STATE), 1)
    zero = jnp.zeros((), jnp.bfloat16)
    tail = jnp.where(which == 0, high, jnp.where(which == 1, mid, jnp.where(which == 2, low, zero)))
    pieces = lax.all_to_all(jnp.concatenate([body, tail], axis=1), SEQ, 0, 0, tiled=True)
    entering = carry_states(pieces)
    entering = lax.all_to_all(entering, SEQ, 0, 0, tiled=True)
    return entering.reshape(heads, P_SIZE, STATE)


def summed_over_tp(value):
    size = lax.axis_size("tp")
    spread = jnp.broadcast_to(value[None], (size, *value.shape))
    return lax.all_to_all(spread, "tp", 0, 0, tiled=True).sum(axis=0)


def mixer_local(
    mixer_input,
    gate_input,
    input_matrix,
    output_matrix,
    step_raw,
    step_bias,
    decay_rate,
    skip_weight,
    conv_mixer,
    conv_input,
    conv_output,
    norm_gain,
):
    reach = CONV - 1
    length, width = mixer_input.shape
    heads = width // P_SIZE
    groups = input_matrix.shape[1] // STATE
    shared = heads // groups
    count = lax.axis_size(SEQ)
    edge = jnp.concatenate(
        [mixer_input[-reach:], input_matrix[-reach:], output_matrix[-reach:]], axis=1
    )
    edge = lax.ppermute(edge, SEQ, [(i, i + 1) for i in range(count - 1)])
    mid = width + input_matrix.shape[1]
    signal = conv_silu(mixer_input, conv_mixer, edge[:, :width]).reshape(length, heads, P_SIZE)
    b_state = conv_silu(input_matrix, conv_input, edge[:, width:mid])
    c_state = conv_silu(output_matrix, conv_output, edge[:, mid:])
    b_state = b_state.reshape(length, groups, STATE)
    c_state = c_state.reshape(length, groups, STATE)
    step_size = jax.nn.softplus(step_raw + step_bias[None, :])
    places = jnp.arange(length, dtype=jnp.int32)
    causal = places[:, None] >= places[None, :]
    log_decay = jnp.cumsum(-step_size * decay_rate[None, :], axis=0)
    by_head = log_decay.T
    spread = jnp.where(causal, by_head[:, :, None] - by_head[:, None, :], 0.0)
    decays = jnp.where(causal, jnp.exp(spread), 0.0)
    coupling = jnp.einsum("tgn,sgn->gts", c_state, b_state)
    mixing = decays * jnp.repeat(coupling, shared, axis=0)
    scaled = signal * step_size[:, :, None]
    closing = jnp.exp(log_decay[-1][None, :] - log_decay)
    weighted = (scaled * closing[:, :, None]).reshape(length, groups, shared * P_SIZE)
    own = jnp.einsum("sgq,sgn->gqn", weighted, b_state).reshape(heads, P_SIZE, STATE)
    entering = entering_state(own, log_decay[-1])
    output = jnp.einsum("hts,shp->thp", mixing, scaled)
    later = jnp.einsum(
        "tgn,gqn->tgq",
        c_state.astype(jnp.bfloat16),
        entering.reshape(groups, shared * P_SIZE, STATE),
        preferred_element_type=jnp.float32,
    ).reshape(length, heads, P_SIZE)
    mixed = output + jnp.exp(log_decay)[:, :, None] * later
    mixed = mixed + skip_weight[None, :, None] * signal
    gated = mixed.reshape(length, width) * jax.nn.silu(gate_input.astype(jnp.float32))
    squares = summed_over_tp(jnp.sum(gated * gated, axis=1))
    scaling = lax.rsqrt(squares / (MH * P_SIZE) + norm_epsilon)
    return (gated * scaling[:, None] * norm_gain[None, :]).astype(jnp.bfloat16)


def shards(
    mixer_input,
    gate_input,
    input_matrix,
    output_matrix,
    step_raw,
    step_bias,
    decay_rate,
    skip_weight,
    conv_mixer,
    conv_input,
    conv_output,
    norm_gain,
    queries,
    keys,
    values,
):
    attention_out = attend_local(queries, keys, values)
    mixer_out = mixer_local(
        mixer_input,
        gate_input,
        input_matrix,
        output_matrix,
        step_raw,
        step_bias,
        decay_rate,
        skip_weight,
        conv_mixer,
        conv_input,
        conv_output,
        norm_gain,
    )
    return (mixer_out, attention_out)


def solution(mesh):
    torus = Mesh(mesh.devices.reshape(2, 4, 8, mesh.shape["tp"]), ("xh", "y", "z", "tp"))
    placed = (
        P(SEQ, "tp"),
        P(SEQ, "tp"),
        P(SEQ, "tp"),
        P(SEQ, "tp"),
        P(SEQ, "tp"),
        P("tp"),
        P("tp"),
        P("tp"),
        P(None, "tp"),
        P(None, "tp"),
        P(None, "tp"),
        P("tp"),
        P(SEQ, "tp"),
        P(SEQ, "tp"),
        P(SEQ, "tp"),
    )
    return jax.shard_map(
        shards, mesh=torus, in_specs=placed, out_specs=(P(SEQ, "tp"), P(SEQ, "tp")), check_vma=False
    )
```

```python
import functools
import math

import jax
import jax.numpy as jnp
from jax import lax
from jax.experimental import pallas as pl
from jax.experimental.pallas import tpu as pltpu
from jax.sharding import Mesh
from jax.sharding import PartitionSpec as P


MH = 128
P_SIZE = 64
STATE = 128
HD = 128
CONV = 4
SEQ = ("xh", "y", "z")

norm_epsilon = 1e-05
lowest_score = -1e30
EXP2_SCALE = math.log2(math.e) / math.sqrt(HD)


def exchanged(value, axes):
    return lax.all_to_all(value, axes, 0, 0, tiled=True)


def conv_silu(raw_rows, weights, history):
    padded = jnp.concatenate([history, raw_rows], axis=0).astype(jnp.float32)
    length = raw_rows.shape[0]
    summed = jnp.zeros((length, raw_rows.shape[1]), jnp.float32)
    for offset in range(weights.shape[0]):
        summed = summed + weights[offset][None, :] * padded[offset : offset + length]
    return jax.nn.silu(summed)


def attend_kernel(parts, opening, closing, *refs):
    here_ref, q_ref = refs[:2]
    kv_refs = refs[2 : 2 + parts]
    refs = refs[2 + parts :]
    if opening:
        old_m_ref = old_l_ref = old_acc_ref = None
    else:
        old_m_ref, old_l_ref, old_acc_ref = refs[:3]
        refs = refs[3:]
    if closing:
        o_ref, s0_ref, s1_ref, m_ref, l_ref, acc_ref = refs
    else:
        m_ref, l_ref, acc_ref, s0_ref, s1_ref = refs
    sides, length, width = q_ref.shape
    rows = 2 * length
    lanes = 2 * HD
    turns = width // lanes
    zs = kv_refs[0].shape[0]
    span = zs * length
    s_refs = (s0_ref, s1_ref)
    if opening:
        m_ref[...] = jnp.full_like(m_ref, lowest_score)
        l_ref[...] = jnp.zeros_like(l_ref)
        acc_ref[...] = jnp.zeros_like(acc_ref)
    else:
        m_ref[...] = old_m_ref[...]
        l_ref[...] = old_l_ref[...]
        acc_ref[...] = old_acc_ref[...]

    def scores(kv_ref, side, line, turn):
        both = q_ref[side, :, turn * lanes : (turn + 1) * lanes]
        q = jnp.concatenate([both[:, :HD], both[:, HD:]], axis=0)
        k = kv_ref[:, line, :, :HD].reshape(span, HD)
        return lax.dot_general(k, q, (((1,), (1,)), ((), ())), preferred_element_type=jnp.float32)

    def update(kv_ref, side, line, turn, s):
        at = side * turns + turn
        m = m_ref[at]
        new = jnp.maximum(m, jnp.max(s, axis=0, keepdims=True))
        p = jnp.exp2((s - new) * EXP2_SCALE)
        factor = jnp.exp2((m - new) * EXP2_SCALE)
        m_ref[at] = new
        l_ref[at] = l_ref[at] * factor + jnp.sum(p, axis=0, keepdims=True)
        v = jnp.concatenate([kv_ref[z, line, :, HD:] for z in range(zs)], axis=1)
        acc_ref[at] = acc_ref[at] * factor + jnp.dot(
            v, p.astype(jnp.bfloat16), preferred_element_type=jnp.float32
        )

    def whole(kv_ref, count):
        def pick(i):
            i = jnp.minimum(i, count - 1)
            return jnp.where(i == 1, 0, 1), jnp.where(i == 2, 1, 0)

        s_refs[0][...] = scores(kv_ref, 1, 0, 0)

        def one(i, _):
            for turn in range(turns):
                if turn < turns - 1:
                    side, line = pick(i)
                    s_refs[1 - turn % 2][...] = scores(kv_ref, side, line, turn + 1)
                else:
                    side, line = pick(i + 1)
                    s_refs[1 - turn % 2][...] = scores(kv_ref, side, line, 0)
                side, line = pick(i)
                update(kv_ref, side, line, turn, s_refs[turn % 2][...])
            return 0

        lax.fori_loop(0, count, one, 0)

    for k in range(parts):
        if opening:
            kv_ref = kv_refs[k]
            place = lax.broadcasted_iota(jnp.int32, (span, rows), 1) % length
            place = place + here_ref[0] * length
            key_row = lax.broadcasted_iota(jnp.int32, (span, rows), 0)
            key_z = (here_ref[0] + zs - key_row // length) % zs
            allowed = key_z * length + key_row % length <= place
            s_refs[0][...] = scores(kv_ref, 0, 0, 0)

            def diagonal(side, _):
                for turn in range(turns):
                    ahead = side if turn < turns - 1 else jnp.minimum(side + 1, sides - 1)
                    s_refs[1 - turn % 2][...] = scores(kv_ref, ahead, ahead, (turn + 1) % turns)
                    s = jnp.where(allowed, s_refs[turn % 2][...], lowest_score)
                    update(kv_ref, side, side, turn, s)
                return 0

            lax.fori_loop(0, sides, diagonal, 0)
            whole(kv_ref, 1)
        else:
            whole(kv_refs[k], jnp.where(here_ref[2 + k] < here_ref[1], 3, 1))

    if closing:

        def close(side, _):
            for turn in range(turns):
                at = side * turns + turn
                out = acc_ref[at] / l_ref[at]
                for pair in range(2):
                    left = turn * lanes + pair * HD
                    piece = out[:, pair * length : (pair + 1) * length]
                    o_ref[side, :, left : left + HD] = piece.T.astype(jnp.bfloat16)
            return 0

        lax.fori_loop(0, sides, close, 0)


def attend(here, q, kvs, state, closing):
    sides, length, width = q.shape
    parts = len(kvs)
    span = kvs[0].shape[0] * length
    rows = 2 * length
    held = sides * width // (2 * HD)
    pairs = parts * 3 * width // HD * length * span
    vmem = pl.BlockSpec(memory_space=pltpu.VMEM)
    kept = [
        ((held, 1, rows), jnp.float32),
        ((held, 1, rows), jnp.float32),
        ((held, HD, rows), jnp.float32),
    ]
    scratch = [pltpu.VMEM((span, rows), jnp.float32)] * 2
    if closing:
        out_shape = jax.ShapeDtypeStruct((sides, length, width), jnp.bfloat16)
        out_specs = vmem
        scratch = scratch + [pltpu.VMEM(*one) for one in kept]
    else:
        out_shape = [jax.ShapeDtypeStruct(*one) for one in kept]
        out_specs = [vmem] * 3
    return pl.pallas_call(
        functools.partial(attend_kernel, parts, not state, closing),
        out_shape=out_shape,
        in_specs=[pl.BlockSpec(memory_space=pltpu.SMEM)] + [vmem] * (1 + parts + len(state)),
        out_specs=out_specs,
        scratch_shapes=scratch,
        cost_estimate=pl.CostEstimate(
            flops=pairs * HD * 4,
            bytes_accessed=parts * kvs[0].size * 2 + q.size * 4,
            transcendentals=pairs,
        ),
        compiler_params=pltpu.CompilerParams(vmem_limit_bytes=14 * 1024 * 1024),
        name="attend",
    )(here, q, *kvs, *state)


def moved(value, axis, by):
    size = lax.axis_size(axis)
    return lax.ppermute(value, axis, [(i, (i + by) % size) for i in range(size)])


def swapped(mine, others):
    first = lax.axis_index("xh") == 0
    given = moved(others, "xh", 1)
    return jnp.where(first, mine, given), jnp.where(first, given, mine)


def chosen(pair, other):
    first = lax.axis_index("xh") == (1 if other else 0)
    return jnp.where(first, pair[0], pair[1])


def prepare_kernel(here_ref, k_ref, v_ref, x_ref, b_ref, c_ref, kept_ref, given_ref, edge_ref):
    first = here_ref[0] == 0
    k = k_ref[...]
    v = v_ref[...]
    blocks = []
    for head in range(2):
        at = slice(head * HD, (head + 1) * HD)
        blocks.append(jnp.concatenate([k[:, at], v[:, at].T], axis=1))
    kept_ref[...] = jnp.where(first, blocks[0], blocks[1])
    given_ref[...] = jnp.where(first, blocks[1], blocks[0])
    reach = edge_ref.shape[0]
    at = 0
    for ref in (x_ref, b_ref, c_ref):
        edge_ref[:, at : at + ref.shape[1]] = ref[ref.shape[0] - reach :]
        at += ref.shape[1]


def prepare(keys, values, mixer_input, input_matrix, output_matrix):
    length, kv_width = keys.shape
    last = length // 16 - 1
    widths = [mixer_input.shape[1], input_matrix.shape[1], output_matrix.shape[1]]
    here = lax.axis_index("xh").astype(jnp.int32).reshape(1)
    whole = pl.BlockSpec((length, kv_width), lambda i: (0, 0))
    return pl.pallas_call(
        prepare_kernel,
        grid=(1,),
        out_shape=[
            jax.ShapeDtypeStruct((length, 2 * HD), keys.dtype),
            jax.ShapeDtypeStruct((length, 2 * HD), keys.dtype),
            jax.ShapeDtypeStruct((CONV - 1, sum(widths)), mixer_input.dtype),
        ],
        in_specs=[pl.BlockSpec(memory_space=pltpu.SMEM), whole, whole]
        + [pl.BlockSpec((16, width), lambda i: (last, 0)) for width in widths],
        out_specs=[
            pl.BlockSpec((length, 2 * HD), lambda i: (0, 0)),
            pl.BlockSpec((length, 2 * HD), lambda i: (0, 0)),
            pl.BlockSpec((CONV - 1, sum(widths)), lambda i: (0, 0)),
        ],
        cost_estimate=pl.CostEstimate(flops=2000000, bytes_accessed=400000, transcendentals=0),
        name="prepare",
    )(here, keys, values, mixer_input, input_matrix, output_matrix)


def pack_kernel(*refs):
    for k, ref in enumerate(refs[:-1]):
        refs[-1][k] = ref[...]


def packed(blocks):
    vmem = pl.BlockSpec(memory_space=pltpu.VMEM)
    total = len(blocks) * blocks[0].size
    return pl.pallas_call(
        pack_kernel,
        out_shape=jax.ShapeDtypeStruct((len(blocks), *blocks[0].shape), blocks[0].dtype),
        in_specs=[vmem] * len(blocks),
        out_specs=vmem,
        cost_estimate=pl.CostEstimate(flops=total, bytes_accessed=4 * total, transcendentals=0),
        compiler_params=pltpu.CompilerParams(vmem_limit_bytes=4 * 1024 * 1024),
        name="pack",
    )(*blocks)


def gathered_keys(kept, given):
    own = jnp.stack(swapped(kept, given))
    ups, downs = [own], [own]
    far = lax.axis_size("z") // 2
    for step in range(1, far + 1):
        ups.append(moved(ups[-1], "z", 1))
        if step < far:
            downs.append(moved(downs[-1], "z", -1))
    return packed(ups + downs[:0:-1])


def carry_kernel(piece_ref, o_ref):
    count, rows = o_ref.shape[0], o_ref.shape[1]

    def step(j, state):
        o_ref[j] = state.astype(jnp.bfloat16)
        block = piece_ref[j].astype(jnp.float32)
        log = block[rows : rows + 1] + block[rows + 1 : rows + 2] + block[rows + 2 : rows + 3]
        return jnp.exp(log) * state + block[:rows]

    lax.fori_loop(0, count, step, jnp.zeros((rows, STATE), jnp.float32), unroll=8)


def carry_states(pieces):
    count, rows = pieces.shape[0], pieces.shape[1] - 8
    return pl.pallas_call(
        carry_kernel,
        out_shape=jax.ShapeDtypeStruct((count, rows, STATE), jnp.bfloat16),
        in_specs=[pl.BlockSpec(memory_space=pltpu.VMEM)],
        out_specs=pl.BlockSpec(memory_space=pltpu.VMEM),
        cost_estimate=pl.CostEstimate(
            flops=1000000, bytes_accessed=pieces.size * 4, transcendentals=count * 128
        ),
        compiler_params=pltpu.CompilerParams(vmem_limit_bytes=4 * 1024 * 1024),
        name="carry_states",
    )(pieces)


def entering_state(own, log_total, first, second):
    heads = own.shape[0]
    count = lax.axis_size(SEQ)
    rows = heads * P_SIZE // count
    per_head = count // heads
    body = own.astype(jnp.bfloat16).reshape(count, rows, STATE)
    log = jnp.repeat(log_total, per_head)[:, None, None]
    high = log.astype(jnp.bfloat16)
    rest = log - high.astype(jnp.float32)
    mid = rest.astype(jnp.bfloat16)
    low = (rest - mid.astype(jnp.float32)).astype(jnp.bfloat16)
    which = lax.broadcasted_iota(jnp.int32, (count, 8, STATE), 1)
    zero = jnp.zeros((), jnp.bfloat16)
    tail = jnp.where(which == 0, high, jnp.where(which == 1, mid, jnp.where(which == 2, low, zero)))
    pieces = jnp.concatenate([body, tail], axis=1)
    pieces = exchanged(pieces, SEQ)
    pieces, first = lax.optimization_barrier((pieces, first))
    entering = carry_states(pieces)
    entering = exchanged(entering, SEQ)
    entering, state = lax.optimization_barrier((entering, second(first)))
    return entering.reshape(heads, P_SIZE, STATE), state


def summed_over_tp(value):
    value = value[None]
    others = [
        lax.ppermute(value, "tp", [(i, i ^ by) for i in range(lax.axis_size("tp"))])
        for by in range(1, lax.axis_size("tp"))
    ]
    return (value + others[0] + others[1] + others[2])[0]


def mixer_local(
    mixer_input,
    gate_input,
    input_matrix,
    output_matrix,
    step_raw,
    step_bias,
    decay_rate,
    skip_weight,
    conv_mixer,
    conv_input,
    conv_output,
    norm_gain,
    edge,
    first,
    second,
):
    length, width = mixer_input.shape
    heads = width // P_SIZE
    groups = input_matrix.shape[1] // STATE
    shared = heads // groups
    count = lax.axis_size(SEQ)
    edge = lax.ppermute(edge, SEQ, [(i, i + 1) for i in range(count - 1)])
    mid = width + input_matrix.shape[1]
    signal = conv_silu(mixer_input, conv_mixer, edge[:, :width]).reshape(length, heads, P_SIZE)
    b_state = conv_silu(input_matrix, conv_input, edge[:, width:mid])
    c_state = conv_silu(output_matrix, conv_output, edge[:, mid:])
    b_state = b_state.reshape(length, groups, STATE)
    c_state = c_state.reshape(length, groups, STATE)
    step_size = jax.nn.softplus(step_raw + step_bias[None, :])
    places = jnp.arange(length, dtype=jnp.int32)
    causal = places[:, None] >= places[None, :]
    log_decay = jnp.cumsum(-step_size * decay_rate[None, :], axis=0)
    by_head = log_decay.T
    spread = jnp.where(causal, by_head[:, :, None] - by_head[:, None, :], 0.0)
    decays = jnp.where(causal, jnp.exp(spread), 0.0)
    coupling = jnp.einsum("tgn,sgn->gts", c_state, b_state)
    mixing = decays * jnp.repeat(coupling, shared, axis=0)
    scaled = signal * step_size[:, :, None]
    closing = jnp.exp(log_decay[-1][None, :] - log_decay)
    weighted = (scaled * closing[:, :, None]).reshape(length, groups, shared * P_SIZE)
    own = jnp.einsum("sgq,sgn->gqn", weighted, b_state).reshape(heads, P_SIZE, STATE)
    entering, first = entering_state(own, log_decay[-1], first, second)
    output = jnp.einsum("hts,shp->thp", mixing, scaled)
    later = jnp.einsum(
        "tgn,gqn->tgq",
        c_state.astype(jnp.bfloat16),
        entering.reshape(groups, shared * P_SIZE, STATE),
        preferred_element_type=jnp.float32,
    ).reshape(length, heads, P_SIZE)
    mixed = output + jnp.exp(log_decay)[:, :, None] * later
    mixed = mixed + skip_weight[None, :, None] * signal
    gated = mixed.reshape(length, width) * jax.nn.silu(gate_input.astype(jnp.float32))
    partial = jnp.sum(gated * gated, axis=1)
    squares = summed_over_tp(partial)
    scaling = lax.rsqrt(squares / (MH * P_SIZE) + norm_epsilon)
    return (gated * scaling[:, None] * norm_gain[None, :]).astype(jnp.bfloat16), first


def shards(
    mixer_input,
    gate_input,
    input_matrix,
    output_matrix,
    step_raw,
    step_bias,
    decay_rate,
    skip_weight,
    conv_mixer,
    conv_input,
    conv_output,
    norm_gain,
    queries,
    keys,
    values,
):
    half = queries.shape[1] // 2
    halves = (queries[:, :half], queries[:, half:])
    q = jnp.stack(swapped(chosen(halves, False), chosen(halves, True)))
    kept, given, edge = prepare(keys, values, mixer_input, input_matrix, output_matrix)
    kv = gathered_keys(kept, given)
    above = moved(kv, "y", 1)
    below = moved(kv, "y", -1)
    near = kv.shape[0] // 2
    far_low = moved(above[:near], "y", 1)
    far_high = moved(below[near:], "y", -1)
    y, ys = lax.axis_index("y"), lax.axis_size("y")
    z = lax.axis_index("z")

    def here(*ups):
        return jnp.stack([z, y] + [(y + up) % ys for up in ups]).astype(jnp.int32)

    state = attend(here(0), q, [kv], [], False)
    mixer_out, state = mixer_local(
        mixer_input,
        gate_input,
        input_matrix,
        output_matrix,
        step_raw,
        step_bias,
        decay_rate,
        skip_weight,
        conv_mixer,
        conv_input,
        conv_output,
        norm_gain,
        edge,
        state,
        lambda state: attend(here(ys - 1, 1), q, [above, below], state, False),
    )
    far = jnp.concatenate([far_low, far_high], axis=0)
    out = attend(here(2), q, [far], state, True)
    halves = swapped(chosen(out, False), chosen(out, True))
    attention_out = jnp.concatenate(halves, axis=1)
    return (mixer_out, attention_out)


def solution(mesh):
    torus = Mesh(mesh.devices.reshape(2, 4, 8, mesh.shape["tp"]), ("xh", "y", "z", "tp"))
    placed = (
        P(SEQ, "tp"),
        P(SEQ, "tp"),
        P(SEQ, "tp"),
        P(SEQ, "tp"),
        P(SEQ, "tp"),
        P("tp"),
        P("tp"),
        P("tp"),
        P(None, "tp"),
        P(None, "tp"),
        P(None, "tp"),
        P("tp"),
        P(SEQ, "tp"),
        P(SEQ, "tp"),
        P(SEQ, "tp"),
    )

    return jax.shard_map(
        shards, mesh=torus, in_specs=placed, out_specs=(P(SEQ, "tp"), P(SEQ, "tp")), check_vma=False
    )
```

```python
import functools
import math

import jax
import jax.numpy as jnp
from jax import lax
from jax.experimental import pallas as pl
from jax.experimental.pallas import tpu as pltpu
from jax.sharding import Mesh
from jax.sharding import PartitionSpec as P


MH = 128
P_SIZE = 64
STATE = 128
HD = 128
CONV = 4
LINE = ("xh", "y")
SEQ = ("xh", "y", "z")

norm_epsilon = 1e-05
lowest_score = -1e30
EXP2_SCALE = math.log2(math.e) / math.sqrt(HD)


def exchanged(value, axes):
    return lax.all_to_all(value, axes, 0, 0, tiled=True)


def attend_kernel(parts, opening, closing, *refs):
    here_ref, q_ref = refs[:2]
    kv_refs = refs[2 : 2 + parts]
    refs = refs[2 + parts :]
    if opening:
        old_m_ref = old_l_ref = old_acc_ref = None
    else:
        old_m_ref, old_l_ref, old_acc_ref = refs[:3]
        refs = refs[3:]
    if closing:
        o_ref, s0_ref, s1_ref, m_ref, l_ref, acc_ref = refs
    else:
        m_ref, l_ref, acc_ref, s0_ref, s1_ref = refs
    sides, length, width = q_ref.shape
    rows = 2 * length
    lanes = 2 * HD
    turns = width // lanes
    zs = kv_refs[0].shape[0]
    span = zs * length
    s_refs = (s0_ref, s1_ref)
    if opening:
        m_ref[...] = jnp.full_like(m_ref, lowest_score)
        l_ref[...] = jnp.zeros_like(l_ref)
        acc_ref[...] = jnp.zeros_like(acc_ref)
    else:
        m_ref[...] = old_m_ref[...]
        l_ref[...] = old_l_ref[...]
        acc_ref[...] = old_acc_ref[...]

    def scores(kv_ref, side, line, turn):
        both = q_ref[side, :, turn * lanes : (turn + 1) * lanes]
        q = jnp.concatenate([both[:, :HD], both[:, HD:]], axis=0)
        k = kv_ref[:, line, :, :HD].reshape(span, HD)
        return lax.dot_general(k, q, (((1,), (1,)), ((), ())), preferred_element_type=jnp.float32)

    def update(kv_ref, side, line, turn, s):
        at = side * turns + turn
        m = m_ref[at]
        new = jnp.maximum(m, jnp.max(s, axis=0, keepdims=True))
        p = jnp.exp2((s - new) * EXP2_SCALE)
        factor = jnp.exp2((m - new) * EXP2_SCALE)
        m_ref[at] = new
        l_ref[at] = l_ref[at] * factor + jnp.sum(p, axis=0, keepdims=True)
        v = jnp.concatenate([kv_ref[z, line, :, HD:] for z in range(zs)], axis=1)
        acc_ref[at] = acc_ref[at] * factor + jnp.dot(
            v, p.astype(jnp.bfloat16), preferred_element_type=jnp.float32
        )

    def whole(kv_ref, count, below):
        def pick(i):
            second = jnp.logical_and(i > 0, count > 1)
            side = jnp.where(jnp.logical_and(second, below), 0, 1)
            return side, jnp.where(jnp.logical_and(second, jnp.logical_not(below)), 1, 0)

        s_refs[0][...] = scores(kv_ref, 1, 0, 0)

        def one(i, _):
            for turn in range(turns):
                if turn < turns - 1:
                    side, line = pick(i)
                    s_refs[1 - turn % 2][...] = scores(kv_ref, side, line, turn + 1)
                else:
                    side, line = pick(i + 1)
                    s_refs[1 - turn % 2][...] = scores(kv_ref, side, line, 0)
                side, line = pick(i)
                update(kv_ref, side, line, turn, s_refs[turn % 2][...])
            return 0

        lax.fori_loop(0, count, one, 0)

    for k in range(parts):
        if opening:
            kv_ref = kv_refs[k]
            place = lax.broadcasted_iota(jnp.int32, (span, rows), 1) % length
            place = place + here_ref[0] * length
            key_row = lax.broadcasted_iota(jnp.int32, (span, rows), 0)
            key_z = (here_ref[0] + zs - key_row // length) % zs
            allowed = key_z * length + key_row % length <= place
            s_refs[0][...] = scores(kv_ref, 0, 0, 0)

            def diagonal(side, _):
                for turn in range(turns):
                    ahead = side if turn < turns - 1 else jnp.minimum(side + 1, sides - 1)
                    s_refs[1 - turn % 2][...] = scores(kv_ref, ahead, ahead, (turn + 1) % turns)
                    s = jnp.where(allowed, s_refs[turn % 2][...], lowest_score)
                    update(kv_ref, side, side, turn, s)
                return 0

            lax.fori_loop(0, sides, diagonal, 0)
            whole(kv_ref, 1, False)
        else:
            whole(kv_refs[k], 2, here_ref[2 + k] < here_ref[1])

    if closing:

        def close(side, _):
            for turn in range(turns):
                at = side * turns + turn
                out = acc_ref[at] / l_ref[at]
                for pair in range(2):
                    left = turn * lanes + pair * HD
                    piece = out[:, pair * length : (pair + 1) * length]
                    o_ref[side, :, left : left + HD] = piece.T.astype(jnp.bfloat16)
            return 0

        lax.fori_loop(0, sides, close, 0)


def attend(here, q, kvs, state, closing):
    sides, length, width = q.shape
    parts = len(kvs)
    span = kvs[0].shape[0] * length
    rows = 2 * length
    held = sides * width // (2 * HD)
    pairs = parts * 3 * width // HD * length * span
    vmem = pl.BlockSpec(memory_space=pltpu.VMEM)
    kept = [
        ((held, 1, rows), jnp.float32),
        ((held, 1, rows), jnp.float32),
        ((held, HD, rows), jnp.float32),
    ]
    scratch = [pltpu.VMEM((span, rows), jnp.float32)] * 2
    if closing:
        out_shape = jax.ShapeDtypeStruct((sides, length, width), jnp.bfloat16)
        out_specs = vmem
        scratch = scratch + [pltpu.VMEM(*one) for one in kept]
    else:
        out_shape = [jax.ShapeDtypeStruct(*one) for one in kept]
        out_specs = [vmem] * 3
    return pl.pallas_call(
        functools.partial(attend_kernel, parts, not state, closing),
        out_shape=out_shape,
        in_specs=[pl.BlockSpec(memory_space=pltpu.SMEM)] + [vmem] * (1 + parts + len(state)),
        out_specs=out_specs,
        scratch_shapes=scratch,
        cost_estimate=pl.CostEstimate(
            flops=pairs * HD * 4,
            bytes_accessed=parts * kvs[0].size * 2 + q.size * 4,
            transcendentals=pairs,
        ),
        compiler_params=pltpu.CompilerParams(vmem_limit_bytes=14 * 1024 * 1024),
        name="attend",
    )(here, q, *kvs, *state)


def moved(value, axis, by):
    size = lax.axis_size(axis)
    return lax.ppermute(value, axis, [(i, (i + by) % size) for i in range(size)])


def swapped(mine, others):
    first = lax.axis_index("xh") == 0
    size = lax.axis_size(LINE)
    given = lax.ppermute(others, LINE, [(i, size - 1 - i) for i in range(size)])
    return jnp.where(first, mine, given), jnp.where(first, given, mine)


def chosen(pair, other):
    first = lax.axis_index("xh") == (1 if other else 0)
    return jnp.where(first, pair[0], pair[1])


def prepare_kernel(here_ref, k_ref, v_ref, x_ref, b_ref, c_ref, kept_ref, given_ref, edge_ref):
    first = here_ref[0] == 0
    k = k_ref[...]
    v = v_ref[...]
    blocks = []
    for head in range(2):
        at = slice(head * HD, (head + 1) * HD)
        blocks.append(jnp.concatenate([k[:, at], v[:, at].T], axis=1))
    kept_ref[...] = jnp.where(first, blocks[0], blocks[1])
    given_ref[...] = jnp.where(first, blocks[1], blocks[0])
    at = 0
    for ref in (x_ref, b_ref, c_ref):
        edge_ref[:, at : at + ref.shape[1]] = ref[8:]
        at += ref.shape[1]


def prepare(keys, values, mixer_input, input_matrix, output_matrix):
    length, kv_width = keys.shape
    last = length // 16 - 1
    widths = [mixer_input.shape[1], input_matrix.shape[1], output_matrix.shape[1]]
    here = lax.axis_index("xh").astype(jnp.int32).reshape(1)
    whole = pl.BlockSpec((length, kv_width), lambda i: (0, 0))
    return pl.pallas_call(
        prepare_kernel,
        grid=(1,),
        out_shape=[
            jax.ShapeDtypeStruct((length, 2 * HD), keys.dtype),
            jax.ShapeDtypeStruct((length, 2 * HD), keys.dtype),
            jax.ShapeDtypeStruct((8, sum(widths)), mixer_input.dtype),
        ],
        in_specs=[pl.BlockSpec(memory_space=pltpu.SMEM), whole, whole]
        + [pl.BlockSpec((16, width), lambda i: (last, 0)) for width in widths],
        out_specs=[
            pl.BlockSpec((length, 2 * HD), lambda i: (0, 0)),
            pl.BlockSpec((length, 2 * HD), lambda i: (0, 0)),
            pl.BlockSpec((8, sum(widths)), lambda i: (0, 0)),
        ],
        cost_estimate=pl.CostEstimate(flops=2000000, bytes_accessed=400000, transcendentals=0),
        name="prepare",
    )(here, keys, values, mixer_input, input_matrix, output_matrix)


def pack_kernel(*refs):
    for k, ref in enumerate(refs[:-1]):
        refs[-1][k] = ref[...]


def packed(blocks):
    vmem = pl.BlockSpec(memory_space=pltpu.VMEM)
    total = len(blocks) * blocks[0].size
    return pl.pallas_call(
        pack_kernel,
        out_shape=jax.ShapeDtypeStruct((len(blocks), *blocks[0].shape), blocks[0].dtype),
        in_specs=[vmem] * len(blocks),
        out_specs=vmem,
        cost_estimate=pl.CostEstimate(flops=total, bytes_accessed=4 * total, transcendentals=0),
        compiler_params=pltpu.CompilerParams(vmem_limit_bytes=4 * 1024 * 1024),
        name="pack",
    )(*blocks)


def gathered_keys(kept, given):
    own = jnp.stack(swapped(kept, given))
    ups, downs = [own], [own]
    far = lax.axis_size("z") // 2
    for step in range(1, far + 1):
        ups.append(moved(ups[-1], "z", 1))
        if step < far:
            downs.append(moved(downs[-1], "z", -1))
    return packed(ups + downs[:0:-1])


def carry_kernel(piece_ref, o_ref):
    count, rows = o_ref.shape[0], o_ref.shape[1]

    def step(j, state):
        o_ref[j] = state.astype(jnp.bfloat16)
        block = piece_ref[j].astype(jnp.float32)
        log = block[rows : rows + 1] + block[rows + 1 : rows + 2] + block[rows + 2 : rows + 3]
        return jnp.exp(log) * state + block[:rows]

    lax.fori_loop(0, count, step, jnp.zeros((rows, STATE), jnp.float32), unroll=8)


def carry_states(pieces):
    count, rows = pieces.shape[0], pieces.shape[1] - 8
    return pl.pallas_call(
        carry_kernel,
        out_shape=jax.ShapeDtypeStruct((count, rows, STATE), jnp.bfloat16),
        in_specs=[pl.BlockSpec(memory_space=pltpu.VMEM)],
        out_specs=pl.BlockSpec(memory_space=pltpu.VMEM),
        cost_estimate=pl.CostEstimate(
            flops=1000000, bytes_accessed=pieces.size * 4, transcendentals=count * 128
        ),
        compiler_params=pltpu.CompilerParams(vmem_limit_bytes=4 * 1024 * 1024),
        name="carry_states",
    )(pieces)


def entering_state(pieces, first, second):
    pieces = exchanged(pieces, SEQ)
    pieces, first = lax.optimization_barrier((pieces, first))
    entering = carry_states(pieces)
    entering = exchanged(entering, SEQ)
    return entering, second(first)


def summed_over_tp(value):
    others = [
        lax.ppermute(value, "tp", [(i, i ^ by) for i in range(lax.axis_size("tp"))])
        for by in range(1, lax.axis_size("tp"))
    ]
    return value + others[0] + others[1] + others[2]


def exact_dot(left, right, dims):
    return lax.dot_general(
        left,
        right,
        (dims, ((), ())),
        precision=lax.Precision.HIGHEST,
        preferred_element_type=jnp.float32,
    )


def spread_heads(values, width):
    heads = values.shape[1]
    shape = (heads, width)
    head = lax.broadcasted_iota(jnp.int32, shape, 0)
    lane = lax.broadcasted_iota(jnp.int32, shape, 1)
    pick = jnp.where(lane // (width // heads) == head, 1.0, 0.0)
    return exact_dot(values, pick, ((1,), (0,)))


def local_kernel(
    x_ref,
    b_ref,
    c_ref,
    edge_ref,
    raw_ref,
    bias_ref,
    rate_ref,
    wx_ref,
    wb_ref,
    wc_ref,
    pieces_ref,
    signal_ref,
    b_out_ref,
    c_out_ref,
    step_ref,
    log_ref,
    turned_ref,
):
    length, width = x_ref.shape
    heads = raw_ref.shape[1]
    groups = b_ref.shape[1] // STATE
    shared = width // groups

    def conv(rows_ref, weights_ref, start, at, size):
        top = edge_ref[:, start + at : start + at + size].astype(jnp.float32)
        rows = rows_ref[:, at : at + size].astype(jnp.float32)
        padded = jnp.concatenate([top, rows], axis=0)
        total = weights_ref[CONV - 1 : CONV, at : at + size] * rows
        for tap in range(CONV - 1):
            low = 8 - (CONV - 1) + tap
            shifted = lax.slice_in_dim(padded, low, low + length, axis=0)
            total = total + weights_ref[tap : tap + 1, at : at + size] * shifted
        return total / (1.0 + jnp.exp(-total))

    raw = raw_ref[...] + bias_ref[...]
    step = jnp.maximum(raw, 0.0) + jnp.log1p(jnp.exp(-jnp.abs(raw)))
    slope = -step * rate_ref[...]
    row = lax.broadcasted_iota(jnp.int32, (length, length), 0)
    column = lax.broadcasted_iota(jnp.int32, (length, length), 1)
    log = exact_dot(jnp.where(column <= row, 1.0, 0.0), slope, ((1,), (0,)))
    turned = exact_dot(slope, jnp.where(row <= column, 1.0, 0.0), ((0,), (0,)))
    whole = exact_dot(slope, jnp.ones((length, STATE), jnp.float32), ((0,), (0,)))
    step_ref[...] = step
    log_ref[...] = log
    turned_ref[...] = turned
    weight = step * jnp.exp(log[length - 1 : length] - log)

    b_state = conv(b_ref, wb_ref, width, 0, groups * STATE).astype(jnp.bfloat16)
    b_out_ref[...] = b_state
    c_out_ref[...] = conv(c_ref, wc_ref, width + groups * STATE, 0, groups * STATE).astype(
        jnp.bfloat16
    )
    factor = spread_heads(weight, width)
    chunk = 512
    for at in range(0, width, chunk):
        signal = conv(x_ref, wx_ref, 0, at, chunk)
        signal_ref[:, at : at + chunk] = signal
        weighted = (signal * factor[:, at : at + chunk]).astype(jnp.bfloat16)
        group = at // shared
        own = lax.dot_general(
            weighted,
            b_state[:, group * STATE : (group + 1) * STATE],
            (((0,), (0,)), ((), ())),
            preferred_element_type=jnp.float32,
        )
        first, last = at // P_SIZE, (at + chunk) // P_SIZE
        rows = pieces_ref.shape[2] - 8
        own = own.reshape(last - first, P_SIZE // rows, rows, STATE).astype(jnp.bfloat16)
        pieces_ref[first:last, :, :rows] = own

    high = whole.astype(jnp.bfloat16).astype(jnp.float32)
    rest = whole - high
    mid = rest.astype(jnp.bfloat16).astype(jnp.float32)
    low = rest - mid
    which = lax.broadcasted_iota(jnp.int32, (heads, 8, STATE), 1)
    high, mid, low = (jnp.broadcast_to(part[:, None], which.shape) for part in (high, mid, low))
    tail = jnp.where(which == 0, high, jnp.where(which == 1, mid, jnp.where(which == 2, low, 0.0)))
    for part in range(pieces_ref.shape[1]):
        pieces_ref[:, part, pieces_ref.shape[2] - 8 :] = tail.astype(jnp.bfloat16)


def tail_kernel(
    signal_ref,
    b_ref,
    c_ref,
    step_ref,
    log_ref,
    turned_ref,
    gate_ref,
    skip_ref,
    entering_ref,
    gated_ref,
    partial_ref,
):
    length, width = signal_ref.shape
    groups = b_ref.shape[1] // STATE
    heads = step_ref.shape[1]
    shared = heads // groups
    row = lax.broadcasted_iota(jnp.int32, (length, length), 0)
    column = lax.broadcasted_iota(jnp.int32, (length, length), 1)
    causal = column <= row
    lane = lax.broadcasted_iota(jnp.int32, (length, 2 * P_SIZE), 1)
    steps = spread_heads(step_ref[...], width)
    reach = spread_heads(jnp.exp(log_ref[...]), width)
    skips = spread_heads(jnp.broadcast_to(skip_ref[...], (8, heads)), width)[:1]
    total = jnp.zeros((length, 2 * P_SIZE), jnp.float32)
    for group in range(groups):
        at = slice(group * STATE, (group + 1) * STATE)
        coupling = lax.dot_general(
            c_ref[:, at], b_ref[:, at], (((1,), (1,)), ((), ())), preferred_element_type=jnp.float32
        )
        later = lax.dot_general(
            c_ref[:, at],
            entering_ref[group * shared * P_SIZE : (group + 1) * shared * P_SIZE],
            (((1,), (1,)), ((), ())),
            preferred_element_type=jnp.float32,
        )
        for pair in range(shared // 2):
            near = slice(pair * 2 * P_SIZE, (pair + 1) * 2 * P_SIZE)
            start = group * shared * P_SIZE + pair * 2 * P_SIZE
            lanes = slice(start, start + 2 * P_SIZE)
            signal = signal_ref[:, lanes]
            scaled = (signal * steps[:, lanes]).astype(jnp.bfloat16)
            sides = []
            for head in range(group * shared + 2 * pair, group * shared + 2 * pair + 2):
                spread = log_ref[:, head : head + 1] - turned_ref[head : head + 1, :]
                decay = jnp.where(causal, jnp.exp(jnp.where(causal, spread, 0.0)), 0.0)
                sides.append(
                    jnp.dot(
                        (decay * coupling).astype(jnp.bfloat16),
                        scaled,
                        preferred_element_type=jnp.float32,
                    )
                )
            mixed = jnp.where(lane < P_SIZE, sides[0], sides[1]) + skips[:, lanes] * signal
            mixed = mixed + reach[:, lanes] * later[:, near]
            gate = gate_ref[:, lanes].astype(jnp.float32)
            gated = mixed * (gate / (1.0 + jnp.exp(-gate)))
            gated_ref[:, lanes] = gated
            total = total + gated * gated
    partial_ref[...] = exact_dot(jnp.ones((8, 2 * P_SIZE), jnp.float32), total, ((1,), (1,)))


def kernel_call(kernel, outs, args, flops):
    vmem = pl.BlockSpec(memory_space=pltpu.VMEM)
    return pl.pallas_call(
        kernel,
        out_shape=[jax.ShapeDtypeStruct(*out) for out in outs],
        in_specs=[vmem] * len(args),
        out_specs=[vmem] * len(outs),
        cost_estimate=pl.CostEstimate(
            flops=flops, bytes_accessed=sum(arg.size * 4 for arg in args), transcendentals=flops // 100
        ),
        compiler_params=pltpu.CompilerParams(vmem_limit_bytes=14 * 1024 * 1024),
    )(*args)


def mixer_local(
    mixer_input,
    gate_input,
    input_matrix,
    output_matrix,
    step_raw,
    step_bias,
    decay_rate,
    skip_weight,
    conv_mixer,
    conv_input,
    conv_output,
    norm_gain,
    edge,
    first,
    second,
):
    length, width = mixer_input.shape
    heads = width // P_SIZE
    states = input_matrix.shape[1]
    count = lax.axis_size(SEQ)
    edge = lax.ppermute(edge, SEQ, [(i, i + 1) for i in range(count - 1)])
    rows = heads * P_SIZE // count
    f32, bf16 = jnp.float32, jnp.bfloat16
    pieces, signal, b_state, c_state, step, log, turned = kernel_call(
        local_kernel,
        [
            ((heads, P_SIZE // rows, rows + 8, STATE), bf16),
            ((length, width), f32),
            ((length, states), bf16),
            ((length, states), bf16),
            ((length, heads), f32),
            ((length, heads), f32),
            ((heads, length), f32),
        ],
        [
            mixer_input,
            input_matrix,
            output_matrix,
            edge,
            step_raw,
            step_bias[None],
            decay_rate[None],
            conv_mixer,
            conv_input,
            conv_output,
        ],
        2000000000,
    )
    pieces = pieces.reshape(count, rows + 8, STATE)
    entering, first = entering_state(pieces, first, second)
    gated, partial = kernel_call(
        tail_kernel,
        [((length, width), f32), ((8, STATE), f32)],
        [
            signal,
            b_state,
            c_state,
            step,
            log,
            turned,
            gate_input,
            skip_weight[None],
            entering.reshape(width, STATE),
        ],
        2000000000,
    )
    squares = summed_over_tp(partial)[0]
    scaling = lax.rsqrt(squares / (MH * P_SIZE) + norm_epsilon)
    return (gated * scaling[:, None] * norm_gain[None, :]).astype(jnp.bfloat16), first


def shards(
    mixer_input,
    gate_input,
    input_matrix,
    output_matrix,
    step_raw,
    step_bias,
    decay_rate,
    skip_weight,
    conv_mixer,
    conv_input,
    conv_output,
    norm_gain,
    queries,
    keys,
    values,
):
    half = queries.shape[1] // 2
    halves = (queries[:, :half], queries[:, half:])
    q = jnp.stack(swapped(chosen(halves, False), chosen(halves, True)))
    kept, given, edge = prepare(keys, values, mixer_input, input_matrix, output_matrix)
    kv = gathered_keys(kept, given)
    above = moved(kv, "y", 1)
    below = moved(kv, "y", -1)
    y, ys = lax.axis_index("y"), lax.axis_size("y")
    z = lax.axis_index("z")

    def here(*ups):
        places = [(y + up) % ys for up in (0, *ups)]
        low = lax.axis_index("xh") == 0
        places = [jnp.where(low, place, ys - 1 - place) for place in places]
        return jnp.stack([z] + places).astype(jnp.int32)

    state = attend(here(0), q, [kv], [], False)
    near = kv.shape[0] // 2
    low_part, high_part = above[:near], below[near:]
    far_low = moved(low_part, "y", 1)
    far_high = moved(high_part, "y", -1)
    mixer_out, state = mixer_local(
        mixer_input,
        gate_input,
        input_matrix,
        output_matrix,
        step_raw,
        step_bias,
        decay_rate,
        skip_weight,
        conv_mixer,
        conv_input,
        conv_output,
        norm_gain,
        edge,
        state,
        lambda state: attend(here(ys - 1, 1), q, [above, below], state, False),
    )
    far = jnp.concatenate([far_low, far_high], axis=0)
    out = attend(here(2), q, [far], state, True)
    halves = swapped(chosen(out, False), chosen(out, True))
    attention_out = jnp.concatenate(halves, axis=1)
    return (mixer_out, attention_out)


def solution(mesh):
    torus = Mesh(mesh.devices.reshape(2, 4, 8, mesh.shape["tp"]), ("xh", "y", "z", "tp"))
    placed = (
        P(SEQ, "tp"),
        P(SEQ, "tp"),
        P(SEQ, "tp"),
        P(SEQ, "tp"),
        P(SEQ, "tp"),
        P("tp"),
        P("tp"),
        P("tp"),
        P(None, "tp"),
        P(None, "tp"),
        P(None, "tp"),
        P("tp"),
        P(SEQ, "tp"),
        P(SEQ, "tp"),
        P(SEQ, "tp"),
    )

    return jax.shard_map(
        shards, mesh=torus, in_specs=placed, out_specs=(P(SEQ, "tp"), P(SEQ, "tp")), check_vma=False
    )
```
